32 devices in a mesh: leaf: 8 (over y, x, core), rhs: 4 (over z).
Axes of the slice: x: 2, y: 2, z: 4, core: 2. Of those that a mesh axis runs over, the one named last changes fastest.
Arguments:
- charges: bfloat16 [65536, 2048], P(('leaf', 'rhs')), may hold values from -6 to 6
- leaf_coef: bfloat16 [128, 256, 512], P(('leaf', 'rhs')), may hold values from -0.25 to 0.25
- leaf_rows: int32 [128, 256], P(('leaf', 'rhs')), may hold values from 0 to 511, as said below
- local_interp: bfloat16 [120, 256, 512], P('leaf'), may hold values from -0.25 to 0.25
- top_interp: bfloat16 [1792, 512], P('leaf'), may hold values from -0.25 to 0.25
Outputs:
- subtree_skel: bfloat16 [2048, 2048], P('leaf', 'rhs')
- top_skel: bfloat16 [1792, 2048], P('leaf', 'rhs')
The draws below stay inside these ranges and needn't reach their ends.
Inputs may be any that keep to these rules, and one draw needn't show every extreme that they name: `leaf_rows`: each row holds 256 distinct positions.
All inputs are finite; a program needn't handle non-finite values.
Results may differ from the reference program's by a relative error of at most 0.012.
Values may be sent and summed in bfloat16 or wider, within the bound.
A program may use at most 64 MiB of HBM per device.

```python
import jax
import jax.numpy as jnp
from jax import lax

S = 256
M = 512
LEAVES_DEV = 16
LEAVES = 128
COLS = 2048
PACK = 224
N_LEAF = 8


def draw_leaf_rows(key, part):
    scores = jax.random.randint(key, (LEAVES, M), 0, 1 << 20) * M + jnp.arange(M, dtype=jnp.int32)[None, :]
    order = jnp.argsort(scores, axis=1, stable=True)
    return order[:, :S].astype(jnp.int32)


def steps_of(own_key, dims, cuts, low, high):
    gain, own = 1.0, jax.random.fold_in(own_key, 6)
    for axis_at, parts in cuts:
        steps = jnp.exp(jax.random.uniform(jax.random.fold_in(own, axis_at), (parts,), jnp.float32, low / len(cuts), high / len(cuts)))
        gain = gain * jnp.repeat(steps, dims[axis_at] // parts).reshape([-1 if axis == axis_at else 1 for axis in range(len(dims))])
    return gain


def scatter_about(own_key, shape, scale, limit, cuts=(), kind=jnp.bfloat16):
    entries = jax.random.normal(own_key, shape, jnp.float32) * scale
    if len(cuts) > 0:
        entries = steps_of(own_key, shape, cuts, -0.22, 0.18) * entries
    return jnp.clip(entries, min=-limit, max=limit).astype(kind)


def setup_inputs(seed: int = 0) -> dict:
    arg_keys = jax.random.split(jax.random.key(seed), 6)
    return {
        "charges": scatter_about(arg_keys[0], (LEAVES * M, COLS), 1.0, 6.0, ((0, 32),)),
        "leaf_coef": scatter_about(arg_keys[1], (LEAVES, S, M), M ** -0.5, 0.25, ((0, 32),)),
        "leaf_rows": draw_leaf_rows(jax.random.fold_in(arg_keys[5], 71), 0),
        "local_interp": scatter_about(arg_keys[3], (N_LEAF * (LEAVES_DEV - 1), S, 2 * S), (2 * S) ** -0.5, 0.25, ((0, 8),)),
        "top_interp": scatter_about(arg_keys[4], (N_LEAF * PACK, 2 * S), (2 * S) ** -0.5, 0.25, ((0, 8),)),
    }


def pick_rows(block, chosen):
    return block[chosen]


def subtree(operand):
    points, coef, chosen, interp = operand
    picked = jax.vmap(pick_rows)(points, chosen).astype(jnp.float32)
    mixed = jnp.einsum("nsm,nmc->nsc", coef.astype(jnp.float32), points.astype(jnp.float32))
    skeleton = (picked + mixed).astype(jnp.bfloat16)
    offset = 0
    node_count = LEAVES_DEV
    while node_count > 1:
        node_count = node_count // 2
        stacked = skeleton.reshape(node_count, 2 * S, COLS)
        matrices = interp[offset:offset + node_count]
        skeleton = jnp.einsum("nij,njc->nic", matrices.astype(jnp.float32), stacked.astype(jnp.float32)).astype(jnp.bfloat16)
        offset = offset + node_count
    return skeleton[0]


def reference(charges, leaf_coef, leaf_rows, local_interp, top_interp):
    points = charges.reshape(N_LEAF, LEAVES_DEV, M, COLS)
    coef = leaf_coef.reshape(N_LEAF, LEAVES_DEV, S, M)
    chosen = leaf_rows.reshape(N_LEAF, LEAVES_DEV, S)
    interp = local_interp.reshape(N_LEAF, LEAVES_DEV - 1, S, 2 * S)
    roots = lax.map(subtree, (points, coef, chosen, interp))
    blocks = top_interp.reshape(N_LEAF, PACK, 2 * S)
    top_levels = N_LEAF.bit_length() - 1
    skeleton = roots
    pieces = []
    for level in range(1, top_levels + 1):
        row_count = S >> level
        offset = S - (S >> (level - 1))
        node_count = N_LEAF >> level
        matrices = blocks[:, offset:offset + row_count].reshape(node_count, S, 2 * S)
        stacked = skeleton.reshape(node_count, 2 * S, COLS)
        skeleton = jnp.einsum("nij,njc->nic", matrices.astype(jnp.float32), stacked.astype(jnp.float32)).astype(jnp.bfloat16)
        pieces.append(skeleton.reshape(N_LEAF, row_count, COLS))
    top_skel = jnp.concatenate(pieces, axis=1).reshape(N_LEAF * PACK, COLS)
    return roots.reshape(N_LEAF * S, COLS), top_skel
```

```python
import functools

import jax
import jax.numpy as jnp
from jax import lax
from jax.experimental import pallas as pl
from jax.experimental.pallas import tpu as pltpu
from jax.sharding import PartitionSpec as P

PARTS = 2


def bit(value, k):
    return (value // (1 << k)) % 2


def flip(value, offset, bits):
    out = 0
    for k in range(bits):
        a, b = bit(value, k), bit(offset, k)
        out = out + (a + b - 2 * a * b) * (1 << k)
    return out


def dot(a, b):
    return jnp.dot(a, b, preferred_element_type=jnp.float32)


def kernel(plan, charges, coef, rows, interp, top, root_out, top_out, *scratch):
    (points, mats, picks, nodes, tops, mixed, first, arrived, merged, stacks,
     load_sem, send_sem, recv_sem, top_send, top_recv) = scratch
    R, L, H, cw = plan["R"], plan["L"], plan["H"], plan["cw"]
    leaves, S, M = plan["leaves"], plan["S"], plan["M"]
    m, n_leaf, early = plan["m"], plan["n_leaf"], plan["early"]
    total = leaves * R
    z = lax.axis_index("rhs")
    p = lax.axis_index("leaf")

    barrier = pltpu.get_barrier_semaphore()
    for b in range(m):
        pl.semaphore_signal(barrier, inc=1, device_id={"rhs": flip(z, 1 << b, m)},
                            device_id_type=pl.DeviceIdType.MESH)
    for delta in range(1, n_leaf):
        pl.semaphore_signal(barrier, inc=1, device_id={"leaf": flip(p, delta, L)},
                            device_id_type=pl.DeviceIdType.MESH)

    chunks = R * H

    def chunk_copy(i):
        column = (flip(z, R - 1 - i // H, m) * H + i % H) * cw
        return pltpu.make_async_copy(
            charges.at[:, pl.ds(pl.multiple_of(column, cw), cw)], points.at[i], load_sem.at[i])

    small = [(rows, picks)] + [(coef.at[n], mats.at[n, pl.ds(0, S)]) for n in range(leaves)]
    where = {}
    late = []
    for level in range(1, early + m + 1):
        count = max(leaves >> level, 1)
        if level <= early:
            start = total - (total >> level - 1) + z * count
        else:
            start = total - (total >> level - 1) + z // (1 << level - early)
        for k in range(count):
            where[level, k] = len(where)
            late.append((interp.at[start + k], nodes.at[where[level, k]]))
    late.append((top, tops))
    loads = [pltpu.make_async_copy(a, b, load_sem.at[chunks + i])
             for i, (a, b) in enumerate(small + late)]
    for copy in loads[:len(small)]:
        copy.start()
    chunk_copy(0).start()
    for copy in loads[len(small):]:
        copy.start()
    for i in range(1, chunks):
        chunk_copy(i).start()

    loads[0].wait()
    lanes = lax.broadcasted_iota(jnp.int32, (S, 128), 1)
    for n in range(leaves):
        across = jnp.transpose(jnp.broadcast_to(picks[n:n + 1, :], (128, S)))
        for t in range(M // 128):
            mats[n, S:, t * 128:(t + 1) * 128] = jnp.where(
                across == lanes + t * 128, 1.0, 0.0).astype(jnp.bfloat16)
    for copy in loads[1:]:
        copy.wait()
    pl.semaphore_wait(barrier, m + n_leaf - 1)

    order = sorted(
        [(b, d, h) for d in range(1, R) for h in range(H) for b in [(d & -d).bit_length() - 1]],
        key=lambda s: (-bin(s[1]).count("1"), s[2], -s[0]))
    slot = {s: i for i, s in enumerate(order)}

    def first_of(d, h):
        return (R - 1 - d) * H + h

    merge_keys = [(b, d, h) for b in range(1, m) for d in range(0, R, 1 << b) for h in range(H)]
    merge_at = {k: i for i, k in enumerate(merge_keys)}

    def held(b, d, h):
        return first.at[first_of(d, h)] if b == 0 else merged.at[merge_at[b, d, h]]

    def send(b, d, h):
        s = slot[b, d, h]
        return pltpu.make_async_remote_copy(
            src_ref=held(b, d, h), dst_ref=arrived.at[s], send_sem=send_sem.at[s],
            recv_sem=recv_sem.at[s], device_id={"rhs": flip(z, 1 << b, m)},
            device_id_type=pl.DeviceIdType.MESH)

    def chunk(i, carry):
        chunk_copy(i).wait()
        for n in range(leaves):
            both = dot(mats[n], points[i, n * M:(n + 1) * M, :])
            mixed[n * S:(n + 1) * S, :] = (both[:S] + both[S:]).astype(jnp.bfloat16)
        for level in range(1, early + 1):
            for k in range(leaves >> level):
                node = dot(nodes[where[level, k]], mixed[2 * k * S:(2 * k + 2) * S, :])
                mixed[k * S:(k + 1) * S, :] = node.astype(jnp.bfloat16)
        first[i] = mixed[:S, :]
        if m:
            for h in range(H):
                @pl.when(i == h)
                def _():
                    send(0, R - 1, h).start()
        return carry

    lax.fori_loop(0, chunks, chunk, 0)

    def merge(b, d, h):
        s = slot[b, d + (1 << b), h]
        send(b, d + (1 << b), h).wait_recv()
        matrix = where[early + b + 1, 0]
        own = bit(z, b)
        mine = nodes[matrix, :, pl.ds(pl.multiple_of(own * S, S), S)]
        other = nodes[matrix, :, pl.ds(pl.multiple_of((1 - own) * S, S), S)]
        return (dot(mine, held(b, d, h)[...]) + dot(other, arrived[s])).astype(jnp.bfloat16)

    done = set()

    def ready(b, d, h):
        if b == 0 or (b, d, h) in done:
            return
        ready(b - 1, d, h)
        merged[merge_at[b, d, h]] = merge(b - 1, d, h)
        done.add((b, d, h))

    for b, d, h in order:
        if d == R - 1:
            continue
        ready(b, d, h)
        send(b, d, h).start()

    def top_copy(level, delta, h):
        group = 1 << level
        height = S >> level - 1
        j = p % group
        mine = stacks.at[level - 1, h, pl.ds(pl.multiple_of(j * height, height), height)]
        index = (group - 2 + delta) * H + h
        return pltpu.make_async_remote_copy(
            src_ref=mine, dst_ref=mine, send_sem=top_send.at[index], recv_sem=top_recv.at[index],
            device_id={"leaf": flip(p, delta, L)}, device_id_type=pl.DeviceIdType.MESH)

    def put(level, h, value):
        height = S >> level - 1
        j = p % (1 << level)
        stacks[level - 1, h, pl.ds(pl.multiple_of(j * height, height), height), :] = value
        for delta in range(1, 1 << level):
            top_copy(level, delta, h).start()

    def begin(h):
        ready(m - 1, 0, h)
        root = merge(m - 1, 0, h) if m else held(0, 0, h)[...]
        root_out[:, h * cw:(h + 1) * cw] = root
        if L:
            put(1, h, root)

    def climb(level, h):
        for delta in range(1, 1 << level):
            top_copy(level, delta, h).wait_recv()
        offset, count = S - (S >> level - 1), S >> level
        value = dot(tops[offset:offset + count, :], stacks[level - 1, h]).astype(jnp.bfloat16)
        top_out[offset:offset + count, h * cw:(h + 1) * cw] = value
        if level < L:
            put(level + 1, h, value)

    for h in range(H):
        begin(h)
        for level in range(1, L + 1):
            climb(level, h)

    for s in order:
        send(*s).wait_send()
    for level in range(1, L + 1):
        for delta in range(1, 1 << level):
            for h in range(H):
                top_copy(level, delta, h).wait_send()


def local(charges, leaf_coef, leaf_rows, local_interp, top_interp):
    R, n_leaf = lax.axis_size("rhs"), lax.axis_size("leaf")
    leaves, S, M = leaf_coef.shape
    cols = charges.shape[1]
    m, L = R.bit_length() - 1, n_leaf.bit_length() - 1
    early = leaves.bit_length() - 1
    H = PARTS
    cw = cols // R // H
    plan = dict(R=R, L=L, H=H, cw=cw, leaves=leaves, S=S, M=M, m=m, n_leaf=n_leaf, early=early)
    node_count = leaves - 1 + m
    merge_count = max(sum(R >> b for b in range(1, m)) * H, 1)
    sends = max((R - 1) * H, 1)
    top_sends = max(sum((1 << l) - 1 for l in range(1, L + 1)), 1)
    top_slots = max(((1 << L) - 2 + (1 << L)) * H, 1)
    bf = jnp.bfloat16
    pack = top_interp.shape[0]
    any_spec = pl.BlockSpec(memory_space=pl.ANY)
    vmem = pl.BlockSpec(memory_space=pltpu.VMEM)
    return pl.pallas_call(
        functools.partial(kernel, plan),
        out_shape=(jax.ShapeDtypeStruct((S, cw * H), bf), jax.ShapeDtypeStruct((pack, cw * H), bf)),
        in_specs=[any_spec] * 5,
        out_specs=(vmem, vmem),
        scratch_shapes=[
            pltpu.VMEM((R * H, leaves * M, cw), bf),
            pltpu.VMEM((leaves, 2 * S, M), bf),
            pltpu.VMEM((leaves, S), jnp.int32),
            pltpu.VMEM((node_count, S, 2 * S), bf),
            pltpu.VMEM((pack, 2 * S), bf),
            pltpu.VMEM((leaves * S, cw), bf),
            pltpu.VMEM((R * H, S, cw), bf),
            pltpu.VMEM((sends, S, cw), bf),
            pltpu.VMEM((merge_count, S, cw), bf),
            pltpu.VMEM((max(L, 1), H, 2 * S, cw), bf),
            pltpu.SemaphoreType.DMA((R * H + 2 + leaves + node_count,)),
            pltpu.SemaphoreType.DMA((sends,)),
            pltpu.SemaphoreType.DMA((sends,)),
            pltpu.SemaphoreType.DMA((top_slots,)),
            pltpu.SemaphoreType.DMA((top_slots,)),
        ],
        compiler_params=pltpu.CompilerParams(collective_id=0, has_side_effects=True,
                                             vmem_limit_bytes=60 * 1024 * 1024),
    )(charges, leaf_coef, leaf_rows, local_interp, top_interp)


def solution(mesh):
    placed = (
        P(("leaf", "rhs"), None),
        P(("leaf", "rhs"), None, None),
        P(("leaf", "rhs"), None),
        P("leaf", None, None),
        P("leaf", None),
    )
    return jax.shard_map(
        local,
        mesh=mesh,
        in_specs=placed,
        out_specs=(P("leaf", "rhs"), P("leaf", "rhs")),
        check_vma=False,
    )
```

```python
import functools

import jax
import jax.numpy as jnp
from jax import lax
from jax.experimental import pallas as pl
from jax.experimental.pallas import tpu as pltpu
from jax.sharding import PartitionSpec as P

PARTS = 2


def bit(value, k):
    return (value // (1 << k)) % 2


def flip(value, offset, bits):
    out = 0
    for k in range(bits):
        a, b = bit(value, k), bit(offset, k)
        out = out + (a + b - 2 * a * b) * (1 << k)
    return out


def dot(a, b):
    return jnp.dot(a, b, preferred_element_type=jnp.float32)


def kernel(plan, charges, coef, rows, interp, top, root_out, top_out, *scratch):
    (points, mats, picks, nodes, tops, mixed, first, arrived, merged,
     tables, pairs, leaving, coming, padded, load_sem, send_sem, recv_sem,
     table_send, table_recv, pair_send, pair_recv, part_send, part_recv) = scratch
    pack = top.shape[0]
    R, L, H, cw = plan["R"], plan["L"], plan["H"], plan["cw"]
    leaves, S, M = plan["leaves"], plan["S"], plan["M"]
    m, n_leaf, early = plan["m"], plan["n_leaf"], plan["early"]
    total = leaves * R
    z = lax.axis_index("rhs")
    p = lax.axis_index("leaf")

    barrier = pltpu.get_barrier_semaphore()
    for b in range(m):
        pl.semaphore_signal(barrier, inc=1, device_id={"rhs": flip(z, 1 << b, m)},
                            device_id_type=pl.DeviceIdType.MESH)
    for delta in range(1, n_leaf):
        pl.semaphore_signal(barrier, inc=1, device_id={"leaf": flip(p, delta, L)},
                            device_id_type=pl.DeviceIdType.MESH)

    chunks = R * H
    fetches = [1] * (L > 0) + list(range(2, n_leaf, 2))

    def table_copy(delta):
        part = pl.ds(0, S // 2) if delta == 1 else pl.ds(S // 2, pack - S // 2)
        k = fetches.index(delta)
        return pltpu.make_async_remote_copy(
            src_ref=top.at[part], dst_ref=tables.at[k, part], send_sem=table_send.at[k],
            recv_sem=table_recv.at[k], device_id={"leaf": flip(p, delta, L)},
            device_id_type=pl.DeviceIdType.MESH)


    def chunk_copy(i):
        column = (flip(z, R - 1 - i // H, m) * H + i % H) * cw
        return pltpu.make_async_copy(
            charges.at[:, pl.ds(pl.multiple_of(column, cw), cw)], points.at[i], load_sem.at[i])

    small = [(rows, picks)] + [(coef.at[n], mats.at[n, pl.ds(0, S)]) for n in range(leaves)]
    where = {}
    late = []
    for level in range(1, early + m + 1):
        count = max(leaves >> level, 1)
        if level <= early:
            start = total - (total >> level - 1) + z * count
        else:
            start = total - (total >> level - 1) + z // (1 << level - early)
        for k in range(count):
            where[level, k] = len(where)
            late.append((interp.at[start + k], nodes.at[where[level, k]]))
    late.append((top, tops))
    loads = [pltpu.make_async_copy(a, b, load_sem.at[chunks + i])
             for i, (a, b) in enumerate(small + late)]
    for copy in loads[:len(small)]:
        copy.start()
    chunk_copy(0).start()
    soon = len(small) + leaves - 1
    for copy in loads[len(small):soon]:
        copy.start()

    loads[0].wait()
    lanes = lax.broadcasted_iota(jnp.int32, (S, 128), 1)
    for n in range(leaves):
        across = jnp.transpose(jnp.broadcast_to(picks[n:n + 1, :], (128, S)))
        for t in range(M // 128):
            mats[n, S:, t * 128:(t + 1) * 128] = jnp.where(
                across == lanes + t * 128, 1.0, 0.0).astype(jnp.bfloat16)
    for i in range(1, chunks):
        chunk_copy(i).start()
    for copy in loads[soon:]:
        copy.start()
    pl.semaphore_wait(barrier, m + n_leaf - 1)
    for delta in fetches:
        table_copy(delta).start()
    for copy in loads[1:soon]:
        copy.wait()

    order = sorted(
        [(b, d, h) for d in range(1, R) for h in range(H) for b in [(d & -d).bit_length() - 1]],
        key=lambda s: (-bin(s[1]).count("1"), s[2], -s[0]))
    slot = {s: i for i, s in enumerate(order)}

    def first_of(d, h):
        return (R - 1 - d) * H + h

    merge_keys = [(b, d, h) for b in range(1, m) for d in range(0, R, 1 << b) for h in range(H)]
    merge_at = {k: i for i, k in enumerate(merge_keys)}

    def held(b, d, h):
        return first.at[first_of(d, h)] if b == 0 else merged.at[merge_at[b, d, h]]

    def send(b, d, h):
        s = slot[b, d, h]
        return pltpu.make_async_remote_copy(
            src_ref=held(b, d, h), dst_ref=arrived.at[s], send_sem=send_sem.at[s],
            recv_sem=recv_sem.at[s], device_id={"rhs": flip(z, 1 << b, m)},
            device_id_type=pl.DeviceIdType.MESH)

    def chunk(i, carry):
        chunk_copy(i).wait()
        for n in range(leaves):
            both = dot(mats[n], points[i, n * M:(n + 1) * M, :])
            mixed[n * S:(n + 1) * S, :] = (both[:S] + both[S:]).astype(jnp.bfloat16)
        for level in range(1, early + 1):
            for k in range(leaves >> level):
                node = dot(nodes[where[level, k]], mixed[2 * k * S:(2 * k + 2) * S, :])
                mixed[k * S:(k + 1) * S, :] = node.astype(jnp.bfloat16)
        first[i] = mixed[:S, :]
        if m:
            for h in range(H):
                @pl.when(i == h)
                def _():
                    send(0, R - 1, h).start()
        return carry

    lax.fori_loop(0, chunks, chunk, 0)
    for copy in loads[soon:-1]:
        copy.wait()

    def merge(b, d, h):
        s = slot[b, d + (1 << b), h]
        send(b, d + (1 << b), h).wait_recv()
        matrix = where[early + b + 1, 0]
        own = bit(z, b)
        mine = nodes[matrix, :, pl.ds(pl.multiple_of(own * S, S), S)]
        other = nodes[matrix, :, pl.ds(pl.multiple_of((1 - own) * S, S), S)]
        return (dot(mine, held(b, d, h)[...]) + dot(other, arrived[s])).astype(jnp.bfloat16)

    done = set()

    def ready(b, d, h):
        if b == 0 or (b, d, h) in done:
            return
        ready(b - 1, d, h)
        merged[merge_at[b, d, h]] = merge(b - 1, d, h)
        done.add((b, d, h))

    for b, d, h in order:
        if d == R - 1:
            continue
        ready(b, d, h)
        send(b, d, h).start()

    def pair_copy(level, h):
        height = S >> level - 1
        mine = pairs.at[level - 1, h, pl.ds(pl.multiple_of(p % 2 * height, height), height)]
        return pltpu.make_async_remote_copy(
            src_ref=mine, dst_ref=mine, send_sem=pair_send.at[level - 1, h],
            recv_sem=pair_recv.at[level - 1, h], device_id={"leaf": flip(p, 1, L)},
            device_id_type=pl.DeviceIdType.MESH)

    def part_copy(level, delta, h):
        i = delta // 2
        height = S >> level
        return pltpu.make_async_remote_copy(
            src_ref=leaving.at[level - 1, i, h, pl.ds(0, height)],
            dst_ref=coming.at[level - 1, i, h, pl.ds(0, height)],
            send_sem=part_send.at[level - 1, i, h], recv_sem=part_recv.at[level - 1, i, h],
            device_id={"leaf": flip(p, delta, L)}, device_id_type=pl.DeviceIdType.MESH)

    def put(level, h, value):
        height = S >> level - 1
        pairs[level - 1, h, pl.ds(pl.multiple_of(p % 2 * height, height), height), :] = value
        pair_copy(level, h).start()

    def begin(h):
        ready(m - 1, 0, h)
        root = merge(m - 1, 0, h) if m else held(0, 0, h)[...]
        root_out[:, h * cw:(h + 1) * cw] = root
        if L:
            put(1, h, root)

    def share(level, matrix, h):
        width = 2 * (S >> level - 1)
        chip = p % (1 << level) // 2
        rows = slice(S - (S >> level - 1), S - (S >> level))
        if width % 128 == 0:
            columns = pl.ds(pl.multiple_of(chip * width, width), width)
            return dot(matrix[rows, columns], pairs[level - 1, h, :width, :])
        padded[...] = jnp.zeros_like(padded)
        padded[pl.ds(pl.multiple_of(chip * width, width), width), :] = pairs[level - 1, h, :width, :]
        return dot(matrix[rows, :], padded[...])

    def climb(level, h):
        offset, count = S - (S >> level - 1), S >> level
        if level != 2:
            pair_copy(level, h).wait_recv()
        if level > 1:
            for delta in range(2, 1 << level, 2):
                leaving[level - 1, delta // 2, h, :count, :] = share(
                    level, tables.at[fetches.index(delta)], h).astype(jnp.bfloat16)
                part_copy(level, delta, h).start()
        value = share(level, tops, h)
        if level == 1 and L > 1:
            other = share(1, tables.at[0], h)
            pairs[1, h, pl.ds(pl.multiple_of((1 - p % 2) * count, count), count), :] = other.astype(jnp.bfloat16)
            pairs[1, h, pl.ds(pl.multiple_of(p % 2 * count, count), count), :] = value.astype(jnp.bfloat16)
        return value

    def finish(level, h, value):
        offset, count = S - (S >> level - 1), S >> level
        for delta in range(2, 1 << level, 2):
            part_copy(level, delta, h).wait_recv()
            value = value + coming[level - 1, delta // 2, h, :count, :].astype(jnp.float32)
        value = value.astype(jnp.bfloat16)
        if 2 <= level < L:
            put(level + 1, h, value)
        top_out[offset:offset + count, h * cw:(h + 1) * cw] = value

    for h in range(H):
        begin(h)
    loads[-1].wait()
    for level in range(1, L + 1):
        if level == 1:
            table_copy(1).wait_recv()
        if level == 2:
            for delta in fetches[1:]:
                table_copy(delta).wait_recv()
        values = [climb(level, h) for h in range(H)]
        for h in range(H):
            finish(level, h, values[h])

    for s in order:
        send(*s).wait_send()
    for delta in fetches:
        table_copy(delta).wait_send()
    for level in range(1, L + 1):
        for h in range(H):
            if level != 2:
                pair_copy(level, h).wait_send()
            for delta in range(2, 1 << level, 2):
                part_copy(level, delta, h).wait_send()


def local(charges, leaf_coef, leaf_rows, local_interp, top_interp):
    R, n_leaf = lax.axis_size("rhs"), lax.axis_size("leaf")
    leaves, S, M = leaf_coef.shape
    cols = charges.shape[1]
    m, L = R.bit_length() - 1, n_leaf.bit_length() - 1
    early = leaves.bit_length() - 1
    H = PARTS
    cw = cols // R // H
    plan = dict(R=R, L=L, H=H, cw=cw, leaves=leaves, S=S, M=M, m=m, n_leaf=n_leaf, early=early)
    node_count = leaves - 1 + m
    merge_count = max(sum(R >> b for b in range(1, m)) * H, 1)
    sends = max((R - 1) * H, 1)
    top_levels, chips = max(L, 1), max(n_leaf // 2, 1)
    bf = jnp.bfloat16
    pack = top_interp.shape[0]
    any_spec = pl.BlockSpec(memory_space=pl.ANY)
    vmem = pl.BlockSpec(memory_space=pltpu.VMEM)
    return pl.pallas_call(
        functools.partial(kernel, plan),
        out_shape=(jax.ShapeDtypeStruct((S, cw * H), bf), jax.ShapeDtypeStruct((pack, cw * H), bf)),
        in_specs=[any_spec] * 5,
        out_specs=(vmem, vmem),
        scratch_shapes=[
            pltpu.VMEM((R * H, leaves * M, cw), bf),
            pltpu.VMEM((leaves, 2 * S, M), bf),
            pltpu.VMEM((leaves, S), jnp.int32),
            pltpu.VMEM((node_count, S, 2 * S), bf),
            pltpu.VMEM((pack, 2 * S), bf),
            pltpu.VMEM((leaves * S, cw), bf),
            pltpu.VMEM((R * H, S, cw), bf),
            pltpu.VMEM((sends, S, cw), bf),
            pltpu.VMEM((merge_count, S, cw), bf),
            pltpu.VMEM((max(n_leaf // 2, 1), pack, 2 * S), bf),
            pltpu.VMEM((top_levels, H, 2 * S, cw), bf),
            pltpu.VMEM((top_levels, chips, H, S // 4, cw), bf),
            pltpu.VMEM((top_levels, chips, H, S // 4, cw), bf),
            pltpu.VMEM((2 * S, cw), bf),
            pltpu.SemaphoreType.DMA((R * H + 2 + leaves + node_count,)),
            pltpu.SemaphoreType.DMA((sends,)),
            pltpu.SemaphoreType.DMA((sends,)),
            pltpu.SemaphoreType.DMA((max(n_leaf // 2, 1),)),
            pltpu.SemaphoreType.DMA((max(n_leaf // 2, 1),)),
            pltpu.SemaphoreType.DMA((top_levels, H)),
            pltpu.SemaphoreType.DMA((top_levels, H)),
            pltpu.SemaphoreType.DMA((top_levels, chips, H)),
            pltpu.SemaphoreType.DMA((top_levels, chips, H)),
        ],
        compiler_params=pltpu.CompilerParams(collective_id=0, has_side_effects=True,
                                             vmem_limit_bytes=60 * 1024 * 1024),
    )(charges, leaf_coef, leaf_rows, local_interp, top_interp)


def solution(mesh):
    placed = (
        P(("leaf", "rhs"), None),
        P(("leaf", "rhs"), None, None),
        P(("leaf", "rhs"), None),
        P("leaf", None, None),
        P("leaf", None),
    )
    return jax.shard_map(
        local,
        mesh=mesh,
        in_specs=placed,
        out_specs=(P("leaf", "rhs"), P("leaf", "rhs")),
        check_vma=False,
    )
```

```python
import functools

import jax
import jax.numpy as jnp
from jax import lax
from jax.experimental import pallas as pl
from jax.experimental.pallas import tpu as pltpu
from jax.sharding import PartitionSpec as P

PARTS = 2


def bit(value, k):
    return (value // (1 << k)) % 2


def flip(value, offset, bits):
    out = 0
    for k in range(bits):
        a, b = bit(value, k), bit(offset, k)
        out = out + (a + b - 2 * a * b) * (1 << k)
    return out


def dot(a, b):
    return jnp.dot(a, b, preferred_element_type=jnp.float32)


def kernel(plan, charges, coef, rows, interp, top, root_out, top_out, *scratch):
    (points, mats, picks, nodes, tops, mixed, first, arrived, merged,
     tables, pairs, leaving, coming, padded, load_sem, send_sem, recv_sem,
     table_send, table_recv, pair_send, pair_recv, part_send, part_recv) = scratch
    pack = top.shape[0]
    R, L, H, cw = plan["R"], plan["L"], plan["H"], plan["cw"]
    leaves, S, M = plan["leaves"], plan["S"], plan["M"]
    m, n_leaf, early = plan["m"], plan["n_leaf"], plan["early"]
    total = leaves * R
    z = lax.axis_index("rhs")
    p = lax.axis_index("leaf")

    barrier = pltpu.get_barrier_semaphore()
    for b in range(m):
        pl.semaphore_signal(barrier, inc=1, device_id={"rhs": flip(z, 1 << b, m)},
                            device_id_type=pl.DeviceIdType.MESH)
    for delta in range(1, n_leaf):
        pl.semaphore_signal(barrier, inc=1, device_id={"leaf": flip(p, delta, L)},
                            device_id_type=pl.DeviceIdType.MESH)

    chunks = R * H
    order = sorted(
        [(b, d, h) for d in range(1, R) for h in range(H) for b in [(d & -d).bit_length() - 1]],
        key=lambda s: (-bin(s[1]).count("1"), s[2], s[0]))
    places = [(d, h) for _, d, h in order] + [(0, h) for h in range(H)]
    fetches = [1] * (L > 0) + list(range(2, n_leaf, 2))

    def table_copy(delta):
        part = pl.ds(0, S // 2) if delta == 1 else pl.ds(S // 2, pack - S // 2)
        k = fetches.index(delta)
        return pltpu.make_async_remote_copy(
            src_ref=top.at[part], dst_ref=tables.at[k, part], send_sem=table_send.at[k],
            recv_sem=table_recv.at[k], device_id={"leaf": flip(p, delta, L)},
            device_id_type=pl.DeviceIdType.MESH)


    def chunk_copy(i):
        d, h = places[i]
        column = (flip(z, d, m) * H + h) * cw
        return pltpu.make_async_copy(
            charges.at[:, pl.ds(pl.multiple_of(column, cw), cw)], points.at[i], load_sem.at[i])

    small = [(rows, picks)] + [(coef.at[n], mats.at[n, pl.ds(0, S)]) for n in range(leaves)]
    where = {}
    late = []
    for level in range(1, early + m + 1):
        count = max(leaves >> level, 1)
        if level <= early:
            start = total - (total >> level - 1) + z * count
        else:
            start = total - (total >> level - 1) + z // (1 << level - early)
        for k in range(count):
            where[level, k] = len(where)
            late.append((interp.at[start + k], nodes.at[where[level, k]]))
    late.append((top, tops))
    loads = [pltpu.make_async_copy(a, b, load_sem.at[chunks + i])
             for i, (a, b) in enumerate(small + late)]
    for copy in loads[:len(small)]:
        copy.start()
    chunk_copy(0).start()
    soon = len(small) + leaves - 1
    for copy in loads[len(small):soon]:
        copy.start()

    loads[0].wait()
    lanes = lax.broadcasted_iota(jnp.int32, (S, 128), 1)
    for n in range(leaves):
        across = jnp.transpose(jnp.broadcast_to(picks[n:n + 1, :], (128, S)))
        for t in range(M // 128):
            mats[n, S:, t * 128:(t + 1) * 128] = jnp.where(
                across == lanes + t * 128, 1.0, 0.0).astype(jnp.bfloat16)
    for i in range(1, chunks):
        chunk_copy(i).start()
    for copy in loads[soon:]:
        copy.start()
    pl.semaphore_wait(barrier, m + n_leaf - 1)
    for delta in fetches:
        table_copy(delta).start()
    for copy in loads[1:soon]:
        copy.wait()

    slot = {s: i for i, s in enumerate(order)}

    def first_of(d, h):
        return places.index((d, h))

    merge_keys = [(b, d, h) for b in range(1, m) for d in range(0, R, 1 << b) for h in range(H)]
    merge_at = {k: i for i, k in enumerate(merge_keys)}

    def held(b, d, h):
        return first.at[first_of(d, h)] if b == 0 else merged.at[merge_at[b, d, h]]

    def send(b, d, h):
        s = slot[b, d, h]
        return pltpu.make_async_remote_copy(
            src_ref=held(b, d, h), dst_ref=arrived.at[s], send_sem=send_sem.at[s],
            recv_sem=recv_sem.at[s], device_id={"rhs": flip(z, 1 << b, m)},
            device_id_type=pl.DeviceIdType.MESH)

    def chunk(i):
        chunk_copy(i).wait()
        for n in range(leaves):
            both = dot(mats[n], points[i, n * M:(n + 1) * M, :])
            mixed[n * S:(n + 1) * S, :] = (both[:S] + both[S:]).astype(jnp.bfloat16)
        for level in range(1, early + 1):
            for k in range(leaves >> level):
                node = dot(nodes[where[level, k]], mixed[2 * k * S:(2 * k + 2) * S, :])
                mixed[k * S:(k + 1) * S, :] = node.astype(jnp.bfloat16)
        first[i] = mixed[:S, :]

    def merge(b, d, h):
        s = slot[b, d + (1 << b), h]
        send(b, d + (1 << b), h).wait_recv()
        matrix = where[early + b + 1, 0]
        own = bit(z, b)
        mine = nodes[matrix, :, pl.ds(pl.multiple_of(own * S, S), S)]
        other = nodes[matrix, :, pl.ds(pl.multiple_of((1 - own) * S, S), S)]
        return (dot(mine, held(b, d, h)[...]) + dot(other, arrived[s])).astype(jnp.bfloat16)

    done = set()

    def ready(b, d, h):
        if b == 0 or (b, d, h) in done:
            return
        ready(b - 1, d, h)
        merged[merge_at[b, d, h]] = merge(b - 1, d, h)
        done.add((b, d, h))

    for i, (b, d, h) in enumerate(order):
        chunk(i)
        if b and not done:
            for copy in loads[soon:-1]:
                copy.wait()
        ready(b, d, h)
        send(b, d, h).start()
    for i in range(len(order), chunks):
        chunk(i)
    if m < 2:
        for copy in loads[soon:-1]:
            copy.wait()

    def pair_copy(level, h):
        height = S >> level - 1
        mine = pairs.at[level - 1, h, pl.ds(pl.multiple_of(p % 2 * height, height), height)]
        return pltpu.make_async_remote_copy(
            src_ref=mine, dst_ref=mine, send_sem=pair_send.at[level - 1, h],
            recv_sem=pair_recv.at[level - 1, h], device_id={"leaf": flip(p, 1, L)},
            device_id_type=pl.DeviceIdType.MESH)

    def part_copy(level, delta, h):
        i = delta // 2
        height = S >> level
        return pltpu.make_async_remote_copy(
            src_ref=leaving.at[level - 1, i, h, pl.ds(0, height)],
            dst_ref=coming.at[level - 1, i, h, pl.ds(0, height)],
            send_sem=part_send.at[level - 1, i, h], recv_sem=part_recv.at[level - 1, i, h],
            device_id={"leaf": flip(p, delta, L)}, device_id_type=pl.DeviceIdType.MESH)

    def put(level, h, value):
        height = S >> level - 1
        pairs[level - 1, h, pl.ds(pl.multiple_of(p % 2 * height, height), height), :] = value
        pair_copy(level, h).start()

    def begin(h):
        ready(m - 1, 0, h)
        root = merge(m - 1, 0, h) if m else held(0, 0, h)[...]
        root_out[:, h * cw:(h + 1) * cw] = root
        if L:
            put(1, h, root)

    def share(level, matrix, h):
        width = 2 * (S >> level - 1)
        chip = p % (1 << level) // 2
        rows = slice(S - (S >> level - 1), S - (S >> level))
        if width % 128 == 0:
            columns = pl.ds(pl.multiple_of(chip * width, width), width)
            return dot(matrix[rows, columns], pairs[level - 1, h, :width, :])
        padded[...] = jnp.zeros_like(padded)
        padded[pl.ds(pl.multiple_of(chip * width, width), width), :] = pairs[level - 1, h, :width, :]
        return dot(matrix[rows, :], padded[...])

    def climb(level, h):
        offset, count = S - (S >> level - 1), S >> level
        if level != 2:
            pair_copy(level, h).wait_recv()
        if level > 1:
            for delta in range(2, 1 << level, 2):
                leaving[level - 1, delta // 2, h, :count, :] = share(
                    level, tables.at[fetches.index(delta)], h).astype(jnp.bfloat16)
                part_copy(level, delta, h).start()
        value = share(level, tops, h)
        if level == 1 and L > 1:
            other = share(1, tables.at[0], h)
            pairs[1, h, pl.ds(pl.multiple_of((1 - p % 2) * count, count), count), :] = other.astype(jnp.bfloat16)
            pairs[1, h, pl.ds(pl.multiple_of(p % 2 * count, count), count), :] = value.astype(jnp.bfloat16)
        return value

    def finish(level, h, value):
        offset, count = S - (S >> level - 1), S >> level
        for delta in range(2, 1 << level, 2):
            part_copy(level, delta, h).wait_recv()
            value = value + coming[level - 1, delta // 2, h, :count, :].astype(jnp.float32)
        value = value.astype(jnp.bfloat16)
        if 2 <= level < L:
            put(level + 1, h, value)
        top_out[offset:offset + count, h * cw:(h + 1) * cw] = value

    for h in range(H):
        begin(h)
    loads[-1].wait()
    for level in range(1, L + 1):
        if level == 1:
            table_copy(1).wait_recv()
        if level == 2:
            for delta in fetches[1:]:
                table_copy(delta).wait_recv()
        values = [climb(level, h) for h in range(H)]
        for h in range(H):
            finish(level, h, values[h])

    for s in order:
        send(*s).wait_send()
    for delta in fetches:
        table_copy(delta).wait_send()
    for level in range(1, L + 1):
        for h in range(H):
            if level != 2:
                pair_copy(level, h).wait_send()
            for delta in range(2, 1 << level, 2):
                part_copy(level, delta, h).wait_send()


def store(root, top, root_out, top_out, sems):
    copies = [pltpu.make_async_copy(root, root_out, sems.at[0]),
              pltpu.make_async_copy(top, top_out, sems.at[1])]
    for copy in copies:
        copy.start()
    for copy in copies:
        copy.wait()


def local(charges, leaf_coef, leaf_rows, local_interp, top_interp):
    R, n_leaf = lax.axis_size("rhs"), lax.axis_size("leaf")
    leaves, S, M = leaf_coef.shape
    cols = charges.shape[1]
    m, L = R.bit_length() - 1, n_leaf.bit_length() - 1
    early = leaves.bit_length() - 1
    H = PARTS
    cw = cols // R // H
    plan = dict(R=R, L=L, H=H, cw=cw, leaves=leaves, S=S, M=M, m=m, n_leaf=n_leaf, early=early)
    node_count = leaves - 1 + m
    merge_count = max(sum(R >> b for b in range(1, m)) * H, 1)
    sends = max((R - 1) * H, 1)
    top_levels, chips = max(L, 1), max(n_leaf // 2, 1)
    bf = jnp.bfloat16
    pack = top_interp.shape[0]
    any_spec = pl.BlockSpec(memory_space=pl.ANY)
    vmem = pl.BlockSpec(memory_space=pltpu.VMEM)
    results = pl.pallas_call(
        functools.partial(kernel, plan),
        out_shape=(jax.ShapeDtypeStruct((S, cw * H), bf), jax.ShapeDtypeStruct((pack, cw * H), bf)),
        in_specs=[any_spec] * 5,
        out_specs=(vmem, vmem),
        scratch_shapes=[
            pltpu.VMEM((R * H, leaves * M, cw), bf),
            pltpu.VMEM((leaves, 2 * S, M), bf),
            pltpu.VMEM((leaves, S), jnp.int32),
            pltpu.VMEM((node_count, S, 2 * S), bf),
            pltpu.VMEM((pack, 2 * S), bf),
            pltpu.VMEM((leaves * S, cw), bf),
            pltpu.VMEM((R * H, S, cw), bf),
            pltpu.VMEM((sends, S, cw), bf),
            pltpu.VMEM((merge_count, S, cw), bf),
            pltpu.VMEM((max(n_leaf // 2, 1), pack, 2 * S), bf),
            pltpu.VMEM((top_levels, H, 2 * S, cw), bf),
            pltpu.VMEM((top_levels, chips, H, S // 4, cw), bf),
            pltpu.VMEM((top_levels, chips, H, S // 4, cw), bf),
            pltpu.VMEM((2 * S, cw), bf),
            pltpu.SemaphoreType.DMA((R * H + 2 + leaves + node_count,)),
            pltpu.SemaphoreType.DMA((sends,)),
            pltpu.SemaphoreType.DMA((sends,)),
            pltpu.SemaphoreType.DMA((max(n_leaf // 2, 1),)),
            pltpu.SemaphoreType.DMA((max(n_leaf // 2, 1),)),
            pltpu.SemaphoreType.DMA((top_levels, H)),
            pltpu.SemaphoreType.DMA((top_levels, H)),
            pltpu.SemaphoreType.DMA((top_levels, chips, H)),
            pltpu.SemaphoreType.DMA((top_levels, chips, H)),
        ],
        compiler_params=pltpu.CompilerParams(collective_id=0, has_side_effects=True,
                                             vmem_limit_bytes=60 * 1024 * 1024),
    )(charges, leaf_coef, leaf_rows, local_interp, top_interp)
    return pl.pallas_call(
        store,
        out_shape=(jax.ShapeDtypeStruct((S, cw * H), bf), jax.ShapeDtypeStruct((pack, cw * H), bf)),
        in_specs=[vmem, vmem],
        out_specs=(any_spec, any_spec),
        scratch_shapes=[pltpu.SemaphoreType.DMA((2,))],
    )(*results)


def solution(mesh):
    placed = (
        P(("leaf", "rhs"), None),
        P(("leaf", "rhs"), None, None),
        P(("leaf", "rhs"), None),
        P("leaf", None, None),
        P("leaf", None),
    )
    return jax.shard_map(
        local,
        mesh=mesh,
        in_specs=placed,
        out_specs=(P("leaf", "rhs"), P("leaf", "rhs")),
        check_vma=False,
    )
```
